256 devices in a mesh: vox: 64 (over x, y, z_hi), fil: 4 (over z_lo, core).
Axes of the slice: x: 4, y: 4, z: 8 (z_hi: 4, z_lo: 2; z = z_hi * 2 + z_lo), core: 2. Of those that a mesh axis runs over, the one named last changes fastest.
Arguments:
- volume: bfloat16 [16, 128, 128, 256], P(None, 'vox', 'fil'), may hold values from -6 to 6
- fine_kernel: bfloat16 [16, 16, 3, 3, 3], replicated, may hold values from -0.3125 to 0.3125
- coarse_kernel: bfloat16 [64, 16, 3, 3, 3], replicated, may hold values from -0.3125 to 0.3125
- coarse_cot: bfloat16 [64, 64, 64, 128], P('fil', 'vox'), may hold values from -0.03125 to 0.03125
Outputs:
- coarse_out: bfloat16 [64, 64, 64, 128], P('fil', 'vox')
- grad_fine: float32 [16, 16, 3, 3, 3], replicated
- grad_coarse: float32 [64, 16, 3, 3, 3], replicated
The draws below stay inside these ranges and needn't reach their ends.
All inputs are finite; a program needn't handle non-finite values.
Results may differ from the reference program's by a relative error of at most 0.006.
Values may be sent and summed in bfloat16 or wider, within the bound.
No kernel may reach another device: no remote copies, remote signals or barrier semaphores. Data moves between devices by JAX's collectives and lax.ppermute only.
A program may use at most 128 MiB of HBM per device.

```python
import jax
import jax.numpy as jnp
from jax import lax

C0 = 16
C1 = 64
NZ = 256
NX = 128
NY = 128


def level_of(rng, dims, cuts, least, high):
    factor_of = 1.0
    for axis_at, shards_of in cuts:
        draws = jax.random.uniform(jax.random.fold_in(jax.random.fold_in(rng, 6), axis_at), (shards_of,), jnp.float32, least / len(cuts), high / len(cuts))
        factor_of = factor_of * jnp.repeat(jnp.exp(draws), dims[axis_at] // shards_of).reshape((-1,) + (1,) * (len(dims) - 1 - axis_at))
    return factor_of


def gaussian(rng, dims, width, reach, cuts=(), kind=jnp.bfloat16):
    level = level_of(rng, dims, cuts, -0.22, 0.18) if cuts else 1.0
    result = jax.random.normal(rng, dims, jnp.float32) * width * level
    return jnp.minimum(jnp.maximum(result, -reach), reach).astype(kind)


def setup_inputs(seed: int = 0) -> dict:
    key_of = jax.random.split(jax.random.key(seed), 5)
    volume = gaussian(key_of[0], (C0, NX, NY, NZ), 1.0, 6.0, ((1, 64), (2, 4)))
    fine_kernel = gaussian(key_of[1], (C0, C0, 3, 3, 3), (C0 * 27) ** -0.5, 0.3125)
    coarse_kernel = gaussian(key_of[2], (C1, C0, 3, 3, 3), (C0 * 27) ** -0.5, 0.3125)
    coarse_cot = gaussian(key_of[3], (C1, NX // 2, NY // 2, NZ // 2), (4.0 * (8.0 / (NX * NY * NZ)) ** 0.5), 0.03125, ((0, 4), (1, 64)))
    return dict(volume=volume, fine_kernel=fine_kernel, coarse_kernel=coarse_kernel, coarse_cot=coarse_cot)


def conv_same(field, kernel):
    out = lax.conv_general_dilated(field.astype(jnp.float32)[None], kernel.astype(jnp.float32), (1, 1, 1), [(1, 1), (1, 1), (1, 1)], dimension_numbers=('NCDHW', 'OIDHW', 'NCDHW'), precision=lax.Precision.HIGHEST, preferred_element_type=jnp.float32)
    return out[0]

def kernel_grad(padded, cotangent):
    outs_count = cotangent.shape[0]
    ins_count = padded.shape[0]
    spans = cotangent.shape[1:]
    flat_cot = cotangent.astype(jnp.float32).reshape(outs_count, -1)
    pieces = []
    for first in range(3):
        for second in range(3):
            for third in range(3):
                window = lax.slice(padded, (0, first, second, third), (ins_count, first + spans[0], second + spans[1], third + spans[2]))
                flat_win = window.astype(jnp.float32).reshape(ins_count, -1)
                pieces.append(lax.dot_general(flat_cot, flat_win, (((1,), (1,)), ((), ())), precision=lax.Precision.HIGHEST, preferred_element_type=jnp.float32))
    stacked = jnp.stack(pieces, 2)
    return stacked.reshape(outs_count, ins_count, 3, 3, 3)

def pool_cubes(field):
    shape = field.shape
    return field.reshape(shape[0], shape[1] // 2, 2, shape[2] // 2, 2, shape[3] // 2, 2).mean(axis=(2, 4, 6))

def upsample(field):
    shape = field.shape
    wide = jnp.broadcast_to(field[:, :, None, :, None, :, None], (shape[0], shape[1], 2, shape[2], 2, shape[3], 2))
    return wide.reshape(shape[0], shape[1] * 2, shape[2] * 2, shape[3] * 2)

def reference(volume, fine_kernel, coarse_kernel, coarse_cot):
    preact = conv_same(volume, fine_kernel)
    pooled = pool_cubes(jnp.maximum(preact, 0.0)).astype(jnp.bfloat16)
    coarse_out = conv_same(pooled, coarse_kernel).astype(jnp.bfloat16)
    pooled_framed = jnp.pad(pooled, ((0, 0), (1, 1), (1, 1), (1, 1)))
    grad_coarse = kernel_grad(pooled_framed, coarse_cot)
    flipped = coarse_kernel[:, :, ::-1, ::-1, ::-1].transpose(1, 0, 2, 3, 4)
    returned = conv_same(coarse_cot, flipped)
    fine_cot = jnp.where(preact > 0, upsample(returned) * 0.125, 0.0).astype(jnp.bfloat16)
    volume_framed = jnp.pad(volume, ((0, 0), (1, 1), (1, 1), (1, 1)))
    grad_fine = kernel_grad(volume_framed, fine_cot)
    return (coarse_out, grad_fine, grad_coarse)
```

```python
import functools

import jax
import jax.numpy as jnp
from jax import lax
from jax.experimental import pallas as pl
from jax.experimental.pallas import tpu as pltpu
from jax.sharding import PartitionSpec as P


F32 = jnp.float32
BF16 = jnp.bfloat16
VMEM = pl.BlockSpec(memory_space=pltpu.VMEM)
HBM = pl.BlockSpec(memory_space=pltpu.HBM)


def dot(a, b):
    return lax.dot_general(a, b, (((1,), (0,)), ((), ())), preferred_element_type=F32)


def dot_t(a, b):
    return lax.dot_general(a, b, (((1,), (1,)), ((), ())), preferred_element_type=F32)


def iota(shape, dim):
    return lax.broadcasted_iota(jnp.int32, shape, dim)


def position():
    return lax.axis_index("fil"), lax.rem(lax.axis_index("vox"), 2)


def swap_matrix():
    row, col = iota((256, 256), 0), iota((256, 256), 1)
    return jnp.where(col == (row % 16) * 16 + row // 16, 1.0, 0.0).astype(BF16)


def roll_left(x, amount):
    return x if amount == 0 else pltpu.roll(x, x.shape[1] - amount, 1)


def moved(x, step):
    if step == 0:
        return x
    width = x.shape[1]
    edge = 0 if step == 1 else width - 1
    return jnp.where(iota(x.shape, 1) == edge, 0.0, pltpu.roll(x, step % width, 1))


def call(body, outs, scratch=(), flops=2_000_000_000, n_in=1, spec=VMEM, name=None):
    specs = [spec] * n_in
    return pl.pallas_call(
        body,
        out_shape=tuple(jax.ShapeDtypeStruct(s, d) for s, d in outs),
        in_specs=specs,
        out_specs=tuple(VMEM for _ in outs),
        scratch_shapes=scratch,
        cost_estimate=pl.CostEstimate(flops=flops, bytes_accessed=1_000_000, transcendentals=0),
        compiler_params=pltpu.CompilerParams(vmem_limit_bytes=32 * 1024 * 1024),
        name=name,
    )


def pack_kernel(vol_hbm, cot_hbm, near_ref, far_ref, pay_ref, vol_ref, cot_ref, sems):
    fil, odd = position()
    loads = [
        pltpu.make_async_copy(vol_hbm, vol_ref, sems.at[0]),
        pltpu.make_async_copy(cot_hbm, cot_ref, sems.at[1]),
    ]
    for load in loads:
        load.start()
    swap = swap_matrix()
    planes = (near_ref, far_ref)
    loads[0].wait()
    for which, v_ref in enumerate(planes):
        x = 1 - odd if which == 0 else odd
        for half in range(2):
            block = vol_ref[:, pl.ds(x, 1), 16 * half : 16 * half + 16, :].reshape(256, 256)
            v_ref[16 * half : 16 * half + 16] = dot(swap, block).astype(BF16).reshape(16, 16, 256)
    loads[1].wait()
    for dest in range(4):
        block = cot_ref[:, 0, 16 * dest : 16 * dest + 16, :].reshape(256, 128)
        rows = dot(swap, block).astype(BF16).reshape(16, 16, 128)
        pay_ref[dest, 1:17] = rows
        if dest < 3:
            pay_ref[dest + 1, 0] = rows[15]
        else:
            pay_ref[0, 0] = jnp.zeros((16, 128), BF16)
        if dest > 0:
            pay_ref[dest - 1, 17] = rows[0]
        else:
            pay_ref[3, 17] = jnp.zeros((16, 128), BF16)
    for dest in range(4):
        for which, v_ref in enumerate(planes):
            for side in range(2):
                at = 18 + 6 * side + 3 * which
                lanes = slice(128 * side, 128 * side + 128)
                rows = jnp.where(dest > fil, v_ref[29:32, :, lanes], v_ref[0:3, :, lanes])
                pay_ref[dest, at : at + 3] = rows


def weights_kernel(fk_ref, ck_ref, w1_ref, w2_ref, w4_ref):
    row, col = iota((64, 256), 0), iota((64, 256), 1)
    for slot in range(2):
        total = None
        for dy in range(3):
            place = jnp.where(col == (row // 16) * 64 + (slot + 2 - dy) * 16 + row % 16, 1.0, 0.0).astype(BF16)
            part = dot(ck_ref[:, dy].reshape(144, 64), place)
            total = part if total is None else total + part
        w1_ref[144 * slot : 144 * slot + 144] = total.astype(BF16)
    row, col = iota((16, 256), 0), iota((16, 256), 1)
    total = None
    for dx in range(3):
        for dy in range(3):
            place = jnp.where(col == row + 64 * dx + 16 * dy, 1.0, 0.0).astype(BF16)
            part = dot(fk_ref[dx, dy].reshape(48, 16), place)
            total = part if total is None else total + part
    for x in range(2):
        for y in range(2):
            amount = 64 * x + 16 * y
            rolled = (pltpu.roll(total, amount, 1) if amount else total).astype(BF16)
            for dz in range(3):
                at = 64 * dz + 32 * x + 16 * y
                w2_ref[at : at + 16] = rolled[16 * dz : 16 * dz + 16]
    eye = jnp.where(iota((64, 64), 0) == iota((64, 64), 1), 1.0, 0.0).astype(BF16)
    zero = jnp.zeros((16, 64), BF16)
    for dz in range(3):
        for slot in range(2):
            rows = []
            for dx in range(4):
                for at in range(4):
                    dy = at - slot
                    rows.append(ck_ref[dx, dy, dz] if dx < 3 and 0 <= dy < 3 else zero)
            at = 128 * dz + 64 * slot
            w4_ref[at : at + 64] = dot_t(eye, jnp.concatenate(rows, 0)).astype(BF16)


def returned_kernel(got_ref, w1_ref, own_ref, near_ref, far_ref):
    fil, odd = position()
    before = jnp.maximum(fil - 1, 0)
    after = jnp.minimum(fil + 1, 3)
    for which, msg_ref in enumerate((near_ref, far_ref)):
        for side in range(2):
            at = 18 + 6 * side + 3 * which
            msg_ref[16 + 3 * side : 19 + 3 * side] = got_ref[before, at : at + 3]
            msg_ref[22 + 3 * side : 25 + 3 * side] = got_ref[after, at : at + 3]

        @pl.when(fil == 0)
        def _():
            msg_ref[16:22] = jnp.zeros((6, 16, 128), BF16)

        @pl.when(fil == 3)
        def _():
            msg_ref[22:28] = jnp.zeros((6, 16, 128), BF16)

    w1 = w1_ref[...]
    for pair in range(8):
        window = got_ref[:, 2 * pair : 2 * pair + 4].reshape(256, 128)
        product = dot(w1, window).reshape(2, 3, 3, 16, 128)
        for slot in range(2):
            low, own, high = [
                moved(product[slot, tx, 0], -1) + product[slot, tx, 1] + moved(product[slot, tx, 2], 1) for tx in range(3)
            ]
            own_ref[2 * pair + slot] = own
            near_ref[2 * pair + slot] = jnp.where(odd == 0, high, low).astype(BF16)
            far_ref[2 * pair + slot] = jnp.where(odd == 0, low, high).astype(BF16)


def window_of(refs, start, count):
    return jnp.concatenate([r[pl.ds(start, 4)].reshape(64, r.shape[-1]) for r in refs][:count], 0)


def planes_of(ref):
    return [ref.at[x] for x in range(4)]


def fine_kernel_body(a_ref, b_ref, c_ref, d_ref, ma_ref, mb_ref, mc_ref, md_ref, w2_ref, pooled_ref, mask_ref, all_ref, sums):
    fil, odd = position()
    messages = (ma_ref, mb_ref, mc_ref, md_ref)
    for k, v_ref in enumerate((a_ref, b_ref, c_ref, d_ref)):
        x = k + odd * (3 - 2 * k)
        all_ref[x, 3:35] = v_ref[...]
        for side in range(2):
            lanes = slice(128 * side, 128 * side + 128)
            all_ref[x, 0:3, :, lanes] = messages[k][16 + 3 * side : 19 + 3 * side]
            all_ref[x, 35:38, :, lanes] = messages[k][22 + 3 * side : 25 + 3 * side]

    def block(b):
        window = window_of(planes_of(all_ref), 2 * b, 4)
        product = dot(w2_ref[...], window)
        preact = moved(product[0:64], 1) + product[64:128] + moved(product[128:192], -1)
        act = jnp.maximum(preact, 0.0)
        sums[b] = (act[0:16] + act[16:32]) + (act[32:48] + act[48:64])
        return preact

    block(0)
    block(17)

    def step(b, carry):
        mask_ref[b - 1] = jnp.where(block(b) > 0, 1.0, 0.0).astype(BF16)
        return carry

    lax.fori_loop(1, 17, step, 0, unroll=2)

    @pl.when(fil == 0)
    def _():
        sums[0] = jnp.zeros((16, 256), F32)

    @pl.when(fil == 3)
    def _():
        sums[17] = jnp.zeros((16, 256), F32)

    total = sums[...].reshape(288, 256)
    high = total.astype(BF16)
    low = (total - high.astype(F32)).astype(BF16)
    pool = jnp.where(iota((256, 128), 0) // 2 == iota((256, 128), 1), 0.125, 0.0).astype(BF16)
    pooled_ref[...] = (dot(high, pool) + dot(low, pool)).astype(BF16).reshape(18, 16, 128)


def fine_grad_kernel(own_ref, low_ref, high_ref, all_ref, mask_ref, out_ref, up, acc):
    total = own_ref[...] + (low_ref[0:16].astype(F32) + high_ref[0:16].astype(F32))
    scaled = (total * 0.125).astype(BF16).reshape(256, 128)
    spread = jnp.where(iota((128, 256), 0) == iota((128, 256), 1) // 2, 1.0, 0.0).astype(BF16)
    up[...] = dot(scaled, spread).reshape(16, 16, 256)
    acc[...] = jnp.zeros_like(acc)

    def step(y, carry):
        row = up[y]
        cot = jnp.concatenate([row] * 4, 0) * mask_ref[y].astype(F32)
        left = jnp.concatenate([moved(cot, -1), cot, moved(cot, 1)], 0).astype(BF16)
        window = window_of(planes_of(all_ref), 2 * y + 2, 4)
        acc[...] += dot_t(left, window)
        return carry

    lax.fori_loop(0, 16, step, 0, unroll=2)
    for t in range(3):
        total = None
        for cell in range(4):
            part = roll_left(acc[64 * t + 16 * cell : 64 * t + 16 * cell + 16], 64 * (cell // 2) + 16 * (cell % 2))
            total = part if total is None else total + part
        out_ref[16 * t : 16 * t + 16] = total


def coarse_kernel_body(near_ref, own_ref, far_ref, got_ref, w4_ref, fine_ref, out_ref, grad_ref, rows_out, acc, slab):
    _, odd = position()
    slab[2 - 2 * odd] = near_ref[...]
    slab[1] = own_ref[...]
    slab[2 * odd] = far_ref[...]
    acc[...] = jnp.zeros_like(acc)
    pad = jnp.zeros((64, 128), BF16)

    def step(pair, carry):
        window = jnp.concatenate([window_of([slab.at[x] for x in range(3)], 2 * pair, 3), pad], 0)
        product = dot(w4_ref[...], window)
        result = moved(product[0:128], 1) + product[128:256] + moved(product[256:384], -1)
        rows_out[pl.ds(2 * pair, 2)] = result.astype(BF16).reshape(2, 64, 128)
        cot = jnp.concatenate([got_ref[:, 2 * pair + 1 + s].reshape(64, 128) for s in range(2)], 0).astype(F32)
        left = jnp.concatenate([moved(cot, -1), cot, moved(cot, 1)], 0).astype(BF16)
        acc[...] += dot_t(left, window)
        return carry

    lax.fori_loop(0, 8, step, 0, unroll=2)
    swap = swap_matrix()
    for dest in range(4):
        block = rows_out[:, 16 * dest : 16 * dest + 16, :].reshape(256, 128)
        out_ref[dest] = dot(swap, block).astype(BF16).reshape(16, 16, 128)
    grad_ref[0:48] = fine_ref[...].astype(BF16)
    for t in range(3):
        total = acc[128 * t : 128 * t + 64] + roll_left(acc[128 * t + 64 : 128 * t + 128], 16)
        grad_ref[48 + 64 * t : 112 + 64 * t] = total.astype(BF16)
    grad_ref[240:256] = jnp.zeros((16, 256), BF16)


def sum_kernel(parts_ref, out_ref):
    total = parts_ref[0].astype(F32)
    for src in range(1, 16):
        total = total + parts_ref[src].astype(F32)
    for dest in range(16):
        out_ref[dest] = total.astype(BF16)


def unpack_kernel(grad_ref, got_ref, fine_ref, coarse_ref, out_ref):
    eye = jnp.where(iota((256, 256), 0) == iota((256, 256), 1), 1.0, 0.0).astype(BF16)
    for dz in range(3):
        block = grad_ref[dz].astype(F32)
        columns = dot_t(eye, grad_ref[3 + 4 * dz : 7 + 4 * dz].reshape(64, 256))
        for dx in range(3):
            for dy in range(3):
                at = 64 * dx + 16 * dy
                fine_ref[dx, dy, dz] = roll_left(block, at)[:, 0:16]
                coarse_ref[dx, dy, dz] = columns[at : at + 16]
    for src in range(4):
        out_ref[:, 0, 16 * src : 16 * src + 16, :] = got_ref[src]


def swapped(near, far):
    count = lax.axis_size("vox")
    first = [(i, i ^ 1) for i in range(count)]
    second = [(i, ((i + 1) ^ 1) - 1) for i in range(1, count - 1)]
    return lax.ppermute(near, "vox", first), lax.ppermute(far, "vox", second)


def exchange(pieces, groups):
    return lax.all_to_all(pieces, ("vox", "fil"), 0, 0, tiled=True, axis_index_groups=groups)


def local(volume, fine_kernel, coarse_kernel, coarse_cot):
    plane = ((32, 16, 256), BF16)
    near, far, pay = call(
        pack_kernel,
        [plane, plane, ((4, 30, 16, 128), BF16)],
        scratch=[pltpu.VMEM(volume.shape, BF16), pltpu.VMEM(coarse_cot.shape, BF16), pltpu.SemaphoreType.DMA((2,))],
        n_in=2,
        spec=HBM,
        name="pack",
    )(volume, coarse_cot)
    near_got, far_got = swapped(near, far)
    got = lax.all_to_all(pay, "fil", 0, 0, tiled=True)
    w1, w2, w4 = call(
        weights_kernel, [((288, 256), BF16), ((192, 256), BF16), ((384, 256), BF16)], n_in=2, name="weights"
    )(fine_kernel.transpose(2, 3, 4, 0, 1), coarse_kernel.transpose(2, 3, 4, 1, 0))
    message = ((28, 16, 128), BF16)
    own, near_msg, far_msg = call(
        returned_kernel, [((16, 16, 128), F32), message, message], n_in=2, name="returned"
    )(got, w1)
    near_msg_got, far_msg_got = swapped(near_msg, far_msg)
    pooled, mask, cells = call(
        fine_kernel_body,
        [((18, 16, 128), BF16), ((16, 64, 256), BF16), ((4, 38, 16, 256), BF16)],
        scratch=[pltpu.VMEM((18, 16, 256), F32)],
        n_in=9,
        name="fine",
    )(far_got, far, near, near_got, far_msg_got, far_msg, near_msg, near_msg_got, w2)
    pooled_near, pooled_far = swapped(pooled, pooled)
    (fine_part,) = call(
        fine_grad_kernel,
        [((48, 256), F32)],
        scratch=[pltpu.VMEM((16, 16, 256), F32), pltpu.VMEM((192, 256), F32)],
        n_in=5,
        name="fine_grad",
    )(own, near_msg_got, far_msg_got, cells, mask)
    out_pieces, grads = call(
        coarse_kernel_body,
        [((4, 16, 16, 128), BF16), ((256, 256), BF16)],
        scratch=[pltpu.VMEM((16, 64, 128), BF16), pltpu.VMEM((384, 256), F32), pltpu.VMEM((3, 18, 16, 128), BF16)],
        n_in=6,
        name="coarse",
    )(pooled_near, pooled, pooled_far, got, w4, fine_part)
    out_got = lax.all_to_all(out_pieces, "fil", 0, 0, tiled=True)
    lines = [[16 * g + j for j in range(16)] for g in range(16)]
    sheets = [[16 * g + j for g in range(16)] for j in range(16)]
    summed = call(sum_kernel, [((16, 16, 256), BF16)], name="sum")
    parts = exchange(grads.reshape(16, 16, 256), lines)
    parts = exchange(summed(parts)[0], sheets)
    spread = exchange(summed(parts)[0], lines)
    grad_fine, grad_coarse, coarse_out = call(
        unpack_kernel,
        [((3, 3, 3, 16, 16), F32), ((3, 3, 3, 16, 64), F32), ((16, 1, 64, 128), BF16)],
        n_in=2,
        name="unpack",
    )(spread, out_got)
    return (coarse_out, grad_fine.transpose(3, 4, 0, 1, 2), grad_coarse.transpose(4, 3, 0, 1, 2))


def solution(mesh):
    in_specs = (P(None, "vox", "fil", None), P(), P(), P("fil", "vox", None, None))
    out_specs = (P("fil", "vox", None, None), P(), P())
    return jax.shard_map(local, mesh=mesh, in_specs=in_specs, out_specs=out_specs, check_vma=False)
```

```python
import functools

import jax
import jax.numpy as jnp
from jax import lax
from jax.experimental import pallas as pl
from jax.experimental.pallas import tpu as pltpu
from jax.sharding import PartitionSpec as P


F32 = jnp.float32
BF16 = jnp.bfloat16
VMEM = pl.BlockSpec(memory_space=pltpu.VMEM)
HBM = pl.BlockSpec(memory_space=pltpu.HBM)


def dot(a, b):
    return lax.dot_general(a, b, (((1,), (0,)), ((), ())), preferred_element_type=F32)


def dot_t(a, b):
    return lax.dot_general(a, b, (((1,), (1,)), ((), ())), preferred_element_type=F32)


def iota(shape, dim):
    return lax.broadcasted_iota(jnp.int32, shape, dim)


def position():
    return lax.axis_index("fil"), lax.rem(lax.axis_index("vox"), 2)


def swap_matrix():
    row, col = iota((256, 256), 0), iota((256, 256), 1)
    return jnp.where(col == (row % 16) * 16 + row // 16, 1.0, 0.0).astype(BF16)


def roll_left(x, amount):
    return x if amount == 0 else pltpu.roll(x, x.shape[1] - amount, 1)


def moved(x, step):
    if step == 0:
        return x
    width = x.shape[1]
    edge = 0 if step == 1 else width - 1
    return jnp.where(iota(x.shape, 1) == edge, 0.0, pltpu.roll(x, step % width, 1))


def call(body, outs, scratch=(), flops=2_000_000_000, n_in=1, spec=VMEM, vmem=32 * 1024 * 1024, name=None):
    specs = [spec] * n_in
    return pl.pallas_call(
        body,
        out_shape=tuple(jax.ShapeDtypeStruct(s, d) for s, d in outs),
        in_specs=specs,
        out_specs=tuple(VMEM for _ in outs),
        scratch_shapes=scratch,
        cost_estimate=pl.CostEstimate(flops=flops, bytes_accessed=1_000_000, transcendentals=0),
        compiler_params=pltpu.CompilerParams(vmem_limit_bytes=vmem),
        name=name,
    )


def pack_kernel(vol_hbm, cot_hbm, near_ref, far_ref, pay_ref, vol_ref, cot_ref, sems):
    fil, odd = position()
    loads = [
        pltpu.make_async_copy(vol_hbm, vol_ref, sems.at[0]),
        pltpu.make_async_copy(cot_hbm, cot_ref, sems.at[1]),
    ]
    for load in loads:
        load.start()
    swap = swap_matrix()
    planes = (near_ref, far_ref)
    loads[0].wait()
    for which, v_ref in enumerate(planes):
        x = 1 - odd if which == 0 else odd
        for half in range(2):
            block = vol_ref[:, pl.ds(x, 1), 16 * half : 16 * half + 16, :].reshape(256, 256)
            v_ref[16 * half : 16 * half + 16] = dot(swap, block).astype(BF16).reshape(16, 16, 256)
    loads[1].wait()
    for dest in range(4):
        block = cot_ref[:, 0, 16 * dest : 16 * dest + 16, :].reshape(256, 128)
        rows = dot(swap, block).astype(BF16).reshape(16, 16, 128)
        pay_ref[dest, 1:17] = rows
        if dest < 3:
            pay_ref[dest + 1, 0] = rows[15]
        else:
            pay_ref[0, 0] = jnp.zeros((16, 128), BF16)
        if dest > 0:
            pay_ref[dest - 1, 17] = rows[0]
        else:
            pay_ref[3, 17] = jnp.zeros((16, 128), BF16)
    for dest in range(4):
        for which, v_ref in enumerate(planes):
            for side in range(2):
                at = 18 + 6 * side + 3 * which
                lanes = slice(128 * side, 128 * side + 128)
                rows = jnp.where(dest > fil, v_ref[29:32, :, lanes], v_ref[0:3, :, lanes])
                pay_ref[dest, at : at + 3] = rows


def weights_kernel(fk_ref, ck_ref, w1_ref, w2_ref, w4_ref):
    row, col = iota((64, 256), 0), iota((64, 256), 1)
    for slot in range(2):
        total = None
        for dy in range(3):
            place = jnp.where(col == (row // 16) * 64 + (slot + 2 - dy) * 16 + row % 16, 1.0, 0.0).astype(BF16)
            part = dot(ck_ref[:, dy].reshape(144, 64), place)
            total = part if total is None else total + part
        w1_ref[144 * slot : 144 * slot + 144] = total.astype(BF16)
    row, col = iota((16, 256), 0), iota((16, 256), 1)
    total = None
    for dx in range(3):
        for dy in range(3):
            place = jnp.where(col == row + 64 * dx + 16 * dy, 1.0, 0.0).astype(BF16)
            part = dot(fk_ref[dx, dy].reshape(48, 16), place)
            total = part if total is None else total + part
    for x in range(2):
        for y in range(2):
            amount = 64 * x + 16 * y
            rolled = (pltpu.roll(total, amount, 1) if amount else total).astype(BF16)
            for dz in range(3):
                at = 64 * dz + 32 * x + 16 * y
                w2_ref[at : at + 16] = rolled[16 * dz : 16 * dz + 16]
    eye = jnp.where(iota((64, 64), 0) == iota((64, 64), 1), 1.0, 0.0).astype(BF16)
    zero = jnp.zeros((16, 64), BF16)
    for dz in range(3):
        for slot in range(2):
            rows = []
            for dx in range(4):
                for at in range(4):
                    dy = at - slot
                    rows.append(ck_ref[dx, dy, dz] if dx < 3 and 0 <= dy < 3 else zero)
            at = 128 * dz + 64 * slot
            w4_ref[at : at + 64] = dot_t(eye, jnp.concatenate(rows, 0)).astype(BF16)


def returned_kernel(got_ref, w1_ref, own_ref, near_ref, far_ref):
    fil, odd = position()
    before = jnp.maximum(fil - 1, 0)
    after = jnp.minimum(fil + 1, 3)
    for which, msg_ref in enumerate((near_ref, far_ref)):
        for side in range(2):
            at = 18 + 6 * side + 3 * which
            msg_ref[16 + 3 * side : 19 + 3 * side] = got_ref[before, at : at + 3]
            msg_ref[22 + 3 * side : 25 + 3 * side] = got_ref[after, at : at + 3]

        @pl.when(fil == 0)
        def _():
            msg_ref[16:22] = jnp.zeros((6, 16, 128), BF16)

        @pl.when(fil == 3)
        def _():
            msg_ref[22:28] = jnp.zeros((6, 16, 128), BF16)

    w1 = w1_ref[...]
    for pair in range(8):
        window = got_ref[:, 2 * pair : 2 * pair + 4].reshape(256, 128)
        product = dot(w1, window).reshape(2, 3, 3, 16, 128)
        for slot in range(2):
            low, own, high = [
                moved(product[slot, tx, 0], -1) + product[slot, tx, 1] + moved(product[slot, tx, 2], 1) for tx in range(3)
            ]
            own_ref[2 * pair + slot] = own
            near_ref[2 * pair + slot] = jnp.where(odd == 0, high, low).astype(BF16)
            far_ref[2 * pair + slot] = jnp.where(odd == 0, low, high).astype(BF16)


def window_of(refs, start, count):
    return jnp.concatenate([r[pl.ds(start, 4)].reshape(64, r.shape[-1]) for r in refs][:count], 0)


def planes_of(ref):
    return [ref.at[x] for x in range(4)]


def fine_kernel_body(a_ref, b_ref, c_ref, d_ref, ma_ref, mb_ref, mc_ref, md_ref, w2_ref, pooled_ref, mask_ref, all_ref, sums):
    fil, odd = position()
    messages = (ma_ref, mb_ref, mc_ref, md_ref)
    for k, v_ref in enumerate((a_ref, b_ref, c_ref, d_ref)):
        x = k + odd * (3 - 2 * k)
        all_ref[x, 3:35] = v_ref[...]
        for side in range(2):
            lanes = slice(128 * side, 128 * side + 128)
            all_ref[x, 0:3, :, lanes] = messages[k][16 + 3 * side : 19 + 3 * side]
            all_ref[x, 35:38, :, lanes] = messages[k][22 + 3 * side : 25 + 3 * side]

    def block(b):
        window = window_of(planes_of(all_ref), 2 * b, 4)
        product = dot(w2_ref[...], window)
        preact = moved(product[0:64], 1) + product[64:128] + moved(product[128:192], -1)
        act = jnp.maximum(preact, 0.0)
        sums[b] = (act[0:16] + act[16:32]) + (act[32:48] + act[48:64])
        return preact

    block(0)
    block(17)

    def step(b, carry):
        mask_ref[b - 1] = jnp.where(block(b) > 0, 1.0, 0.0).astype(BF16)
        return carry

    lax.fori_loop(1, 17, step, 0, unroll=True)

    @pl.when(fil == 0)
    def _():
        sums[0] = jnp.zeros((16, 256), F32)

    @pl.when(fil == 3)
    def _():
        sums[17] = jnp.zeros((16, 256), F32)

    total = sums[...].reshape(288, 256)
    high = total.astype(BF16)
    low = (total - high.astype(F32)).astype(BF16)
    pool = jnp.where(iota((256, 128), 0) // 2 == iota((256, 128), 1), 0.125, 0.0).astype(BF16)
    pooled_ref[...] = (dot(high, pool) + dot(low, pool)).astype(BF16).reshape(18, 16, 128)


def fine_grad_kernel(own_ref, low_ref, high_ref, all_ref, mask_ref, out_ref, up, acc):
    total = own_ref[...] + (low_ref[0:16].astype(F32) + high_ref[0:16].astype(F32))
    scaled = (total * 0.125).astype(BF16).reshape(256, 128)
    spread = jnp.where(iota((128, 256), 0) == iota((128, 256), 1) // 2, 1.0, 0.0).astype(BF16)
    up[...] = dot(scaled, spread).reshape(16, 16, 256)
    acc[...] = jnp.zeros_like(acc)

    def step(y, carry):
        row = up[y]
        cot = jnp.concatenate([row] * 4, 0) * mask_ref[y].astype(F32)
        left = jnp.concatenate([moved(cot, -1), cot, moved(cot, 1)], 0).astype(BF16)
        window = window_of(planes_of(all_ref), 2 * y + 2, 4)
        acc[...] += dot_t(left, window)
        return carry

    lax.fori_loop(0, 16, step, 0, unroll=True)
    for t in range(3):
        total = None
        for cell in range(4):
            part = roll_left(acc[64 * t + 16 * cell : 64 * t + 16 * cell + 16], 64 * (cell // 2) + 16 * (cell % 2))
            total = part if total is None else total + part
        out_ref[16 * t : 16 * t + 16] = total


def coarse_kernel_body(near_ref, own_ref, far_ref, got_ref, w4_ref, fine_ref, out0_ref, out1_ref, out2_ref, out3_ref, grad_ref, rows_out, acc, slab):
    fil, odd = position()
    slab[2 - 2 * odd] = near_ref[...]
    slab[1] = own_ref[...]
    slab[2 * odd] = far_ref[...]
    acc[...] = jnp.zeros_like(acc)
    pad = jnp.zeros((64, 128), BF16)

    def step(pair, carry):
        window = jnp.concatenate([window_of([slab.at[x] for x in range(3)], 2 * pair, 3), pad], 0)
        product = dot(w4_ref[...], window)
        result = moved(product[0:128], 1) + product[128:256] + moved(product[256:384], -1)
        result = result.astype(BF16).reshape(2, 4, 16, 128)
        for dest in range(4):
            rows_out[dest, pl.ds(2 * pair, 2)] = result[:, dest]
        cot = jnp.concatenate([got_ref[:, 2 * pair + 1 + s].reshape(64, 128) for s in range(2)], 0).astype(F32)
        left = jnp.concatenate([moved(cot, -1), cot, moved(cot, 1)], 0).astype(BF16)
        acc[...] += dot_t(left, window)
        return carry

    lax.fori_loop(0, 8, step, 0, unroll=True)
    swap = swap_matrix()
    for k, out_ref in enumerate((out0_ref, out1_ref, out2_ref, out3_ref)):
        block = rows_out[lax.bitwise_xor(fil, k)].reshape(256, 128)
        out_ref[...] = dot(swap, block).astype(BF16).reshape(16, 16, 128)
    grad_ref[0:48] = fine_ref[...].astype(BF16)
    for t in range(3):
        total = acc[128 * t : 128 * t + 64] + roll_left(acc[128 * t + 64 : 128 * t + 128], 16)
        grad_ref[48 + 64 * t : 112 + 64 * t] = total.astype(BF16)
    grad_ref[240:256] = jnp.zeros((16, 256), BF16)


def sum_kernel(parts_ref, out_ref):
    total = parts_ref[0].astype(F32)
    for src in range(1, 16):
        total = total + parts_ref[src].astype(F32)
    for dest in range(16):
        out_ref[dest] = total.astype(BF16)


def unpack_kernel(grad_ref, got0_ref, got1_ref, got2_ref, got3_ref, fine_ref, coarse_ref, out_ref):
    fil, _ = position()
    eye = jnp.where(iota((256, 256), 0) == iota((256, 256), 1), 1.0, 0.0).astype(BF16)
    for dz in range(3):
        block = grad_ref[dz].astype(F32)
        columns = dot_t(eye, grad_ref[3 + 4 * dz : 7 + 4 * dz].reshape(64, 256))
        for dx in range(3):
            for dy in range(3):
                at = 64 * dx + 16 * dy
                fine_ref[dx, dy, dz] = roll_left(block, at)[:, 0:16]
                coarse_ref[dx, dy, dz] = columns[at : at + 16]
    for k, got_ref in enumerate((got0_ref, got1_ref, got2_ref, got3_ref)):
        at = pl.multiple_of(16 * lax.bitwise_xor(fil, k), 16)
        out_ref[:, 0, pl.ds(at, 16), :] = got_ref[...]


def swapped(near, far):
    count = lax.axis_size("vox")
    first = [(i, i ^ 1) for i in range(count)]
    second = [(i, ((i + 1) ^ 1) - 1) for i in range(1, count - 1)]
    return lax.ppermute(near, "vox", first), lax.ppermute(far, "vox", second)


def exchange(pieces, groups):
    return lax.all_to_all(pieces, ("vox", "fil"), 0, 0, tiled=True, axis_index_groups=groups)


def local(volume, fine_kernel, coarse_kernel, coarse_cot):
    plane = ((32, 16, 256), BF16)
    near, far, pay = call(
        pack_kernel,
        [plane, plane, ((4, 30, 16, 128), BF16)],
        scratch=[pltpu.VMEM(volume.shape, BF16), pltpu.VMEM(coarse_cot.shape, BF16), pltpu.SemaphoreType.DMA((2,))],
        n_in=2,
        spec=HBM,
        vmem=63 * 1024 * 1024,
        name="pack",
    )(volume, coarse_cot)
    near_got, far_got = swapped(near, far)
    got = lax.all_to_all(pay, "fil", 0, 0, tiled=True)
    w1, w2, w4 = call(
        weights_kernel, [((288, 256), BF16), ((192, 256), BF16), ((384, 256), BF16)], n_in=2, name="weights"
    )(fine_kernel.transpose(2, 3, 4, 0, 1), coarse_kernel.transpose(2, 3, 4, 1, 0))
    message = ((28, 16, 128), BF16)
    own, near_msg, far_msg = call(
        returned_kernel, [((16, 16, 128), F32), message, message], n_in=2, name="returned"
    )(got, w1)
    near_msg_got, far_msg_got = swapped(near_msg, far_msg)
    pooled, mask, cells = call(
        fine_kernel_body,
        [((18, 16, 128), BF16), ((16, 64, 256), BF16), ((4, 38, 16, 256), BF16)],
        scratch=[pltpu.VMEM((18, 16, 256), F32)],
        n_in=9,
        name="fine",
    )(far_got, far, near, near_got, far_msg_got, far_msg, near_msg, near_msg_got, w2)
    pooled_near, pooled_far = swapped(pooled, pooled)
    (fine_part,) = call(
        fine_grad_kernel,
        [((48, 256), F32)],
        scratch=[pltpu.VMEM((16, 16, 256), F32), pltpu.VMEM((192, 256), F32)],
        n_in=5,
        name="fine_grad",
    )(own, near_msg_got, far_msg_got, cells, mask)
    *out_pieces, grads = call(
        coarse_kernel_body,
        [((16, 16, 128), BF16)] * 4 + [((256, 256), BF16)],
        scratch=[pltpu.VMEM((4, 16, 16, 128), BF16), pltpu.VMEM((384, 256), F32), pltpu.VMEM((3, 18, 16, 128), BF16)],
        n_in=6,
        name="coarse",
    )(pooled_near, pooled, pooled_far, got, w4, fine_part)
    out_got = out_pieces[:1] + [
        lax.ppermute(out_pieces[k], "fil", [(i, i ^ k) for i in range(4)]) for k in range(1, 4)
    ]
    lines = [[16 * g + j for j in range(16)] for g in range(16)]
    sheets = [[16 * g + j for g in range(16)] for j in range(16)]
    summed = call(sum_kernel, [((16, 16, 256), BF16)], name="sum")
    parts = exchange(grads.reshape(16, 16, 256), lines)
    parts = exchange(summed(parts)[0], sheets)
    spread = exchange(summed(parts)[0], lines)
    grad_fine, grad_coarse, coarse_out = call(
        unpack_kernel,
        [((3, 3, 3, 16, 16), F32), ((3, 3, 3, 16, 64), F32), ((16, 1, 64, 128), BF16)],
        n_in=5,
        name="unpack",
    )(spread, *out_got)
    return (coarse_out, grad_fine.transpose(3, 4, 0, 1, 2), grad_coarse.transpose(4, 3, 0, 1, 2))


def solution(mesh):
    in_specs = (P(None, "vox", "fil", None), P(), P(), P("fil", "vox", None, None))
    out_specs = (P("fil", "vox", None, None), P(), P())
    return jax.shard_map(local, mesh=mesh, in_specs=in_specs, out_specs=out_specs, check_vma=False)
```

```python
import jax
import jax.numpy as jnp
from jax import lax
from jax.experimental import pallas as pl
from jax.experimental.pallas import tpu as pltpu
from jax.sharding import PartitionSpec as P


F32 = jnp.float32
BF16 = jnp.bfloat16
VMEM = pl.BlockSpec(memory_space=pltpu.VMEM)
HBM = pl.BlockSpec(memory_space=pltpu.HBM)


def dot(a, b):
    return lax.dot_general(a, b, (((1,), (0,)), ((), ())), preferred_element_type=F32)


def dot_t(a, b):
    return lax.dot_general(a, b, (((1,), (1,)), ((), ())), preferred_element_type=F32)


def iota(shape, dim):
    return lax.broadcasted_iota(jnp.int32, shape, dim)


def position():
    return lax.axis_index("fil"), lax.rem(lax.axis_index("vox"), 2)


def swap_matrix():
    row, col = iota((256, 256), 0), iota((256, 256), 1)
    return jnp.where(col == (row % 16) * 16 + row // 16, 1.0, 0.0).astype(BF16)


def roll_left(x, amount):
    return x if amount == 0 else pltpu.roll(x, x.shape[1] - amount, 1)


def moved(x, step):
    if step == 0:
        return x
    width = x.shape[1]
    edge = 0 if step == 1 else width - 1
    return jnp.where(iota(x.shape, 1) == edge, 0.0, pltpu.roll(x, step % width, 1))


def call(body, outs, scratch=(), flops=2_000_000_000, n_in=1, spec=VMEM, unread=0, vmem=32 * 1024 * 1024):
    specs = [spec] * n_in + [pl.BlockSpec(memory_space=pl.ANY)] * unread
    return pl.pallas_call(
        body,
        out_shape=tuple(jax.ShapeDtypeStruct(s, d) for s, d in outs),
        in_specs=specs,
        out_specs=tuple(VMEM for _ in outs),
        scratch_shapes=scratch,
        cost_estimate=pl.CostEstimate(flops=flops, bytes_accessed=1_000_000, transcendentals=0),
        compiler_params=pltpu.CompilerParams(vmem_limit_bytes=vmem),
    )


def pack_kernel(vol_hbm, near_ref, far_ref, edge1_ref, edge3_ref, vol_ref, sem):
    fil, odd = position()
    load = pltpu.make_async_copy(vol_hbm, vol_ref, sem.at[0])
    load.start()
    swap = swap_matrix()
    load.wait()
    for which, v_ref in enumerate((near_ref, far_ref)):
        x = 1 - odd if which == 0 else odd
        for half in range(2):
            block = vol_ref[:, pl.ds(x, 1), 16 * half : 16 * half + 16, :].reshape(256, 256)
            v_ref[16 * half : 16 * half + 16] = dot(swap, block).astype(BF16).reshape(16, 16, 256)
        low, high = v_ref[0:3], v_ref[29:32]
        edge1_ref[3 * which : 3 * which + 3] = jnp.where(lax.rem(fil, 2) == 0, high, low)
        edge3_ref[3 * which : 3 * which + 3] = jnp.where(fil < 2, high, low)


def pack_cot_kernel(cot_ref, after_ref, pay_ref):
    swap = swap_matrix()
    for dest in range(4):
        block = cot_ref[:, 0, 16 * dest : 16 * dest + 16, :].reshape(256, 128)
        rows = dot(swap, block).astype(BF16).reshape(16, 16, 128)
        pay_ref[dest, 1:17] = rows
        if dest < 3:
            pay_ref[dest + 1, 0] = rows[15]
        else:
            pay_ref[0, 0] = jnp.zeros((16, 128), BF16)
        if dest > 0:
            pay_ref[dest - 1, 17] = rows[0]
        else:
            pay_ref[3, 17] = jnp.zeros((16, 128), BF16)


def extend_kernel(near_ref, far_ref, edge1_ref, edge3_ref, near_out, far_out):
    fil, _ = position()
    upper = lax.rem(fil, 2) == 1
    for which, (v_ref, out_ref) in enumerate(((near_ref, near_out), (far_ref, far_out))):
        rows = slice(3 * which, 3 * which + 3)
        out_ref[3:35] = v_ref[...]
        out_ref[0:3] = jnp.where(upper, edge1_ref[rows], edge3_ref[rows])
        out_ref[35:38] = jnp.where(upper, edge3_ref[rows], edge1_ref[rows])


def returned_weights(ck_ref):
    row, col = iota((64, 256), 0), iota((64, 256), 1)
    slots = []
    for slot in range(2):
        total = None
        for dy in range(3):
            place = jnp.where(col == (row // 16) * 64 + (slot + 2 - dy) * 16 + row % 16, 1.0, 0.0).astype(BF16)
            part = dot(ck_ref[:, dy].reshape(144, 64), place)
            total = part if total is None else total + part
        slots.append(total.astype(BF16))
    return jnp.concatenate(slots, 0)


def fine_weights_kernel(fk_ref, w2_ref):
    row, col = iota((16, 256), 0), iota((16, 256), 1)
    total = None
    for dx in range(3):
        for dy in range(3):
            place = jnp.where(col == row + 64 * dx + 16 * dy, 1.0, 0.0).astype(BF16)
            part = dot(fk_ref[dx, dy].reshape(48, 16), place)
            total = part if total is None else total + part
    for x in range(2):
        for y in range(2):
            amount = 64 * x + 16 * y
            rolled = (pltpu.roll(total, amount, 1) if amount else total).astype(BF16)
            for dz in range(3):
                at = 64 * dz + 32 * x + 16 * y
                w2_ref[at : at + 16] = rolled[16 * dz : 16 * dz + 16]


def coarse_weights_kernel(ck_ref, after_ref, w4_ref):
    eye = jnp.where(iota((64, 64), 0) == iota((64, 64), 1), 1.0, 0.0).astype(BF16)
    zero = jnp.zeros((16, 64), BF16)
    for dz in range(3):
        for slot in range(2):
            rows = []
            for dx in range(4):
                for at in range(4):
                    dy = at - slot
                    rows.append(ck_ref[dx, dy, dz] if dx < 3 and 0 <= dy < 3 else zero)
            at = 128 * dz + 64 * slot
            w4_ref[at : at + 64] = dot_t(eye, jnp.concatenate(rows, 0)).astype(BF16)


def returned_kernel(got_ref, ck_ref, pooled_ref, own_ref, near_ref, far_ref):
    _, odd = position()
    near_ref[0:18] = pooled_ref[...]
    far_ref[0:18] = pooled_ref[...]
    w1 = returned_weights(ck_ref)
    for pair in range(8):
        window = got_ref[:, 2 * pair : 2 * pair + 4].reshape(256, 128)
        product = dot(w1, window).reshape(2, 3, 3, 16, 128)
        for slot in range(2):
            low, own, high = [
                moved(product[slot, tx, 0], -1) + product[slot, tx, 1] + moved(product[slot, tx, 2], 1) for tx in range(3)
            ]
            own_ref[2 * pair + slot] = own
            near_ref[18 + 2 * pair + slot] = jnp.where(odd == 0, high, low).astype(BF16)
            far_ref[18 + 2 * pair + slot] = jnp.where(odd == 0, low, high).astype(BF16)


def window_of(refs, start, count):
    return jnp.concatenate([r[pl.ds(start, 4)].reshape(64, r.shape[-1]) for r in refs][:count], 0)


def planes_of(ref):
    return [ref.at[x] for x in range(4)]


def fine_kernel_body(a_ref, b_ref, c_ref, d_ref, w2_ref, pooled_ref, mask_ref, all_ref, sums):
    fil, odd = position()
    for k, v_ref in enumerate((a_ref, b_ref, c_ref, d_ref)):
        all_ref[k + odd * (3 - 2 * k)] = v_ref[...]

    def block(b):
        window = window_of(planes_of(all_ref), 2 * b, 4)
        product = dot(w2_ref[...], window)
        preact = moved(product[0:64], 1) + product[64:128] + moved(product[128:192], -1)
        act = jnp.maximum(preact, 0.0)
        sums[b] = (act[0:16] + act[16:32]) + (act[32:48] + act[48:64])
        return preact

    block(0)
    block(17)

    def step(b, carry):
        mask_ref[b - 1] = jnp.where(block(b) > 0, 1.0, 0.0).astype(BF16)
        return carry

    lax.fori_loop(1, 17, step, 0, unroll=True)

    @pl.when(fil == 0)
    def _():
        sums[0] = jnp.zeros((16, 256), F32)

    @pl.when(fil == 3)
    def _():
        sums[17] = jnp.zeros((16, 256), F32)

    total = sums[...].reshape(288, 256)
    high = total.astype(BF16)
    low = (total - high.astype(F32)).astype(BF16)
    pool = jnp.where(iota((256, 128), 0) // 2 == iota((256, 128), 1), 0.125, 0.0).astype(BF16)
    pooled_ref[...] = (dot(high, pool) + dot(low, pool)).astype(BF16).reshape(18, 16, 128)


def fine_grad_part(own_ref, near_msg, far_msg, all_ref, mask_ref, out_ref, up, acc):
    total = own_ref[...] + (near_msg[18:34].astype(F32) + far_msg[18:34].astype(F32))
    scaled = (total * 0.125).astype(BF16).reshape(256, 128)
    spread = jnp.where(iota((128, 256), 0) == iota((128, 256), 1) // 2, 1.0, 0.0).astype(BF16)
    up[...] = dot(scaled, spread).reshape(16, 16, 256)
    acc[...] = jnp.zeros_like(acc)

    def step(y, carry):
        row = up[y]
        cot = jnp.concatenate([row] * 4, 0) * mask_ref[y].astype(F32)
        left = jnp.concatenate([moved(cot, -1), cot, moved(cot, 1)], 0).astype(BF16)
        window = window_of(planes_of(all_ref), 2 * y + 2, 4)
        acc[...] += dot_t(left, window)
        return carry

    lax.fori_loop(0, 16, step, 0, unroll=True)
    for t in range(3):
        total = None
        for cell in range(4):
            part = roll_left(acc[64 * t + 16 * cell : 64 * t + 16 * cell + 16], 64 * (cell // 2) + 16 * (cell % 2))
            total = part if total is None else total + part
        out_ref[16 * t : 16 * t + 16] = total


def last_kernel(
    own_r, near_msg, own_msg, far_msg, got_ref, all_ref, mask_ref, w4_ref,
    out0_ref, out1_ref, out2_ref, out3_ref, grad_ref, rows_out, acc, slab, up, fine_acc, fine_ref,
):
    fil, odd = position()
    fine_grad_part(own_r, near_msg, far_msg, all_ref, mask_ref, fine_ref, up, fine_acc)
    slab[2 - 2 * odd] = near_msg[0:18]
    slab[1] = own_msg[0:18]
    slab[2 * odd] = far_msg[0:18]
    acc[...] = jnp.zeros_like(acc)
    pad = jnp.zeros((64, 128), BF16)

    def step(pair, carry):
        window = jnp.concatenate([window_of([slab.at[x] for x in range(3)], 2 * pair, 3), pad], 0)
        product = dot(w4_ref[...], window)
        result = moved(product[0:128], 1) + product[128:256] + moved(product[256:384], -1)
        result = result.astype(BF16).reshape(2, 4, 16, 128)
        for dest in range(4):
            rows_out[dest, pl.ds(2 * pair, 2)] = result[:, dest]
        cot = jnp.concatenate([got_ref[:, 2 * pair + 1 + s].reshape(64, 128) for s in range(2)], 0).astype(F32)
        left = jnp.concatenate([moved(cot, -1), cot, moved(cot, 1)], 0).astype(BF16)
        acc[...] += dot_t(left, window)
        return carry

    lax.fori_loop(0, 8, step, 0, unroll=True)
    swap = swap_matrix()
    for k, out_ref in enumerate((out0_ref, out1_ref, out2_ref, out3_ref)):
        block = rows_out[lax.bitwise_xor(fil, k)].reshape(256, 128)
        out_ref[...] = dot(swap, block).astype(BF16).reshape(16, 16, 128)
    grad_ref[0:48] = fine_ref[...].astype(BF16)
    for t in range(3):
        total = acc[128 * t : 128 * t + 64] + roll_left(acc[128 * t + 64 : 128 * t + 128], 16)
        grad_ref[48 + 64 * t : 112 + 64 * t] = total.astype(BF16)
    grad_ref[240:256] = jnp.zeros((16, 256), BF16)


def sum_kernel(parts_ref, out_ref):
    total = parts_ref[0].astype(F32)
    for src in range(1, 16):
        total = total + parts_ref[src].astype(F32)
    for dest in range(16):
        out_ref[dest] = total.astype(BF16)


def unpack_kernel(grad_ref, got0_ref, got1_ref, got2_ref, got3_ref, fine_ref, coarse_ref, out_ref):
    fil, _ = position()
    eye = jnp.where(iota((256, 256), 0) == iota((256, 256), 1), 1.0, 0.0).astype(BF16)
    for dz in range(3):
        block = grad_ref[dz].astype(F32)
        columns = dot_t(eye, grad_ref[3 + 4 * dz : 7 + 4 * dz].reshape(64, 256))
        for dx in range(3):
            for dy in range(3):
                at = 64 * dx + 16 * dy
                fine_ref[dx, dy, dz] = roll_left(block, at)[:, 0:16]
                coarse_ref[dx, dy, dz] = columns[at : at + 16]
    for k, got_ref in enumerate((got0_ref, got1_ref, got2_ref, got3_ref)):
        at = pl.multiple_of(16 * lax.bitwise_xor(fil, k), 16)
        out_ref[:, 0, pl.ds(at, 16), :] = got_ref[...]


def swapped(near, far):
    count = lax.axis_size("vox")
    first = [(i, i ^ 1) for i in range(count)]
    second = [(i, ((i + 1) ^ 1) - 1) for i in range(1, count - 1)]
    near = lax.ppermute(near, "vox", first)
    far = lax.ppermute(far, "vox", second)
    return near, far


def exchange(pieces, groups):
    return lax.all_to_all(pieces, ("vox", "fil"), 0, 0, tiled=True, axis_index_groups=groups)


def local(volume, fine_kernel, coarse_kernel, coarse_cot):
    plane, edge, wide = ((32, 16, 256), BF16), ((6, 16, 256), BF16), ((38, 16, 256), BF16)
    near, far, edge1, edge3 = call(
        pack_kernel,
        [plane, plane, edge, edge],
        scratch=[pltpu.VMEM(volume.shape, BF16), pltpu.SemaphoreType.DMA((1,))],
        n_in=1,
        spec=HBM,
    )(volume)
    (pay,) = call(pack_cot_kernel, [((4, 18, 16, 128), BF16)], n_in=1, unread=1)(coarse_cot, edge1)
    edge1 = lax.ppermute(edge1, "fil", [(i, i ^ 1) for i in range(4)])
    edge3 = lax.ppermute(edge3, "fil", [(1, 2), (2, 1)])
    got = lax.all_to_all(pay, "fil", 0, 0, tiled=True)
    near, far = call(extend_kernel, [wide, wide], n_in=4)(near, far, edge1, edge3)
    near_got, far_got = swapped(near, far)
    (w2,) = call(fine_weights_kernel, [((192, 256), BF16)], n_in=1)(fine_kernel.transpose(2, 3, 4, 0, 1))
    coarse_taps = coarse_kernel.transpose(2, 3, 4, 1, 0)
    pooled, mask, cells = call(
        fine_kernel_body,
        [((18, 16, 128), BF16), ((16, 64, 256), BF16), ((4, 38, 16, 256), BF16)],
        scratch=[pltpu.VMEM((18, 16, 256), F32)],
        n_in=5,
    )(far_got, far, near, near_got, w2)
    message = ((34, 16, 128), BF16)
    own_r, near_msg, far_msg = call(
        returned_kernel, [((16, 16, 128), F32), message, message], n_in=3
    )(got, coarse_taps, pooled)
    (w4,) = call(coarse_weights_kernel, [((384, 256), BF16)], n_in=1, unread=1)(coarse_taps, near_msg)
    near_msg_got, far_msg_got = swapped(near_msg, far_msg)
    *out_pieces, grads = call(
        last_kernel,
        [((16, 16, 128), BF16)] * 4 + [((256, 256), BF16)],
        scratch=[
            pltpu.VMEM((4, 16, 16, 128), BF16),
            pltpu.VMEM((384, 256), F32),
            pltpu.VMEM((3, 18, 16, 128), BF16),
            pltpu.VMEM((16, 16, 256), F32),
            pltpu.VMEM((192, 256), F32),
            pltpu.VMEM((48, 256), F32),
        ],
        n_in=8,
    )(own_r, near_msg_got, near_msg, far_msg_got, got, cells, mask, w4)
    out_got = out_pieces[:1] + [
        lax.ppermute(out_pieces[k], "fil", [(i, i ^ k) for i in range(4)]) for k in range(1, 4)
    ]
    lines = [[16 * g + j for j in range(16)] for g in range(16)]
    sheets = [[16 * g + j for g in range(16)] for j in range(16)]
    summed = call(sum_kernel, [((16, 16, 256), BF16)])
    parts = exchange(grads.reshape(16, 16, 256), lines)
    parts = exchange(summed(parts)[0], sheets)
    spread = exchange(summed(parts)[0], lines)
    grad_fine, grad_coarse, coarse_out = call(
        unpack_kernel, [((3, 3, 3, 16, 16), F32), ((3, 3, 3, 16, 64), F32), ((16, 1, 64, 128), BF16)], n_in=5
    )(spread, *out_got)
    return (coarse_out, grad_fine.transpose(3, 4, 0, 1, 2), grad_coarse.transpose(4, 3, 0, 1, 2))


def solution(mesh):
    in_specs = (P(None, "vox", "fil", None), P(), P(), P("fil", "vox", None, None))
    out_specs = (P("fil", "vox", None, None), P(), P())
    return jax.shard_map(local, mesh=mesh, in_specs=in_specs, out_specs=out_specs, check_vma=False)
```

```python
import jax
import jax.numpy as jnp
from jax import lax
from jax.experimental import pallas as pl
from jax.experimental.pallas import tpu as pltpu
from jax.sharding import PartitionSpec as P


F32 = jnp.float32
BF16 = jnp.bfloat16
VMEM = pl.BlockSpec(memory_space=pltpu.VMEM)
HBM = pl.BlockSpec(memory_space=pltpu.HBM)


def dot(a, b):
    return lax.dot_general(a, b, (((1,), (0,)), ((), ())), preferred_element_type=F32)


def dot_t(a, b):
    return lax.dot_general(a, b, (((1,), (1,)), ((), ())), preferred_element_type=F32)


def iota(shape, dim):
    return lax.broadcasted_iota(jnp.int32, shape, dim)


def position():
    return lax.axis_index("fil"), lax.rem(lax.axis_index("vox"), 2)


def swap_matrix():
    row, col = iota((256, 256), 0), iota((256, 256), 1)
    return jnp.where(col == (row % 16) * 16 + row // 16, 1.0, 0.0).astype(BF16)


def roll_left(x, amount):
    return x if amount == 0 else pltpu.roll(x, x.shape[1] - amount, 1)


def moved(x, step):
    if step == 0:
        return x
    width = x.shape[1]
    edge = 0 if step == 1 else width - 1
    return jnp.where(iota(x.shape, 1) == edge, 0.0, pltpu.roll(x, step % width, 1))


def call(body, outs, scratch=(), flops=2_000_000_000, n_in=1, spec=VMEM, unread=0, vmem=32 * 1024 * 1024):
    specs = [spec] * n_in + [pl.BlockSpec(memory_space=pl.ANY)] * unread
    return pl.pallas_call(
        body,
        out_shape=tuple(jax.ShapeDtypeStruct(s, d) for s, d in outs),
        in_specs=specs,
        out_specs=tuple(VMEM for _ in outs),
        scratch_shapes=scratch,
        cost_estimate=pl.CostEstimate(flops=flops, bytes_accessed=1_000_000, transcendentals=0),
        compiler_params=pltpu.CompilerParams(vmem_limit_bytes=vmem),
    )


def pack_kernel(vol_hbm, near_ref, far_ref, edge1_ref, edge3_ref, vol_ref, sem):
    fil, odd = position()
    load = pltpu.make_async_copy(vol_hbm, vol_ref, sem.at[0])
    load.start()
    swap = swap_matrix()
    load.wait()
    for which, v_ref in enumerate((near_ref, far_ref)):
        x = 1 - odd if which == 0 else odd
        for half in range(2):
            block = vol_ref[:, pl.ds(x, 1), 16 * half : 16 * half + 16, :].reshape(256, 256)
            v_ref[16 * half : 16 * half + 16] = dot(swap, block).astype(BF16).reshape(16, 16, 256)
        low, high = v_ref[0:3], v_ref[29:32]
        edge1_ref[3 * which : 3 * which + 3] = jnp.where(lax.rem(fil, 2) == 0, high, low)
        edge3_ref[3 * which : 3 * which + 3] = jnp.where(fil < 2, high, low)


def pack_cot_kernel(cot_ref, after_ref, pay_ref):
    swap = swap_matrix()
    for dest in range(4):
        block = cot_ref[:, 0, 16 * dest : 16 * dest + 16, :].reshape(256, 128)
        rows = dot(swap, block).astype(BF16).reshape(16, 16, 128)
        pay_ref[dest, 1:17] = rows
        if dest < 3:
            pay_ref[dest + 1, 0] = rows[15]
        else:
            pay_ref[0, 0] = jnp.zeros((16, 128), BF16)
        if dest > 0:
            pay_ref[dest - 1, 17] = rows[0]
        else:
            pay_ref[3, 17] = jnp.zeros((16, 128), BF16)


def extend_kernel(near_ref, far_ref, edge1_ref, edge3_ref, near_out, far_out):
    fil, _ = position()
    upper = lax.rem(fil, 2) == 1
    for which, (v_ref, out_ref) in enumerate(((near_ref, near_out), (far_ref, far_out))):
        rows = slice(3 * which, 3 * which + 3)
        out_ref[3:35] = v_ref[...]
        out_ref[0:3] = jnp.where(upper, edge1_ref[rows], edge3_ref[rows])
        out_ref[35:38] = jnp.where(upper, edge3_ref[rows], edge1_ref[rows])


def returned_weights(ck_ref):
    row, col = iota((64, 256), 0), iota((64, 256), 1)
    slots = []
    for slot in range(2):
        total = None
        for dy in range(3):
            place = jnp.where(col == (row // 16) * 64 + (slot + 2 - dy) * 16 + row % 16, 1.0, 0.0).astype(BF16)
            part = dot(ck_ref[:, dy].reshape(144, 64), place)
            total = part if total is None else total + part
        slots.append(total.astype(BF16))
    return jnp.concatenate(slots, 0)


def fine_weights_kernel(fk_ref, w2_ref):
    row, col = iota((16, 256), 0), iota((16, 256), 1)
    total = None
    for dx in range(3):
        for dy in range(3):
            place = jnp.where(col == row + 64 * dx + 16 * dy, 1.0, 0.0).astype(BF16)
            part = dot(fk_ref[dx, dy].reshape(48, 16), place)
            total = part if total is None else total + part
    for x in range(2):
        for y in range(2):
            amount = 64 * x + 16 * y
            rolled = (pltpu.roll(total, amount, 1) if amount else total).astype(BF16)
            for dz in range(3):
                at = 64 * dz + 32 * x + 16 * y
                w2_ref[at : at + 16] = rolled[16 * dz : 16 * dz + 16]


def coarse_weights_kernel(ck_ref, after_ref, w4_ref):
    eye = jnp.where(iota((64, 64), 0) == iota((64, 64), 1), 1.0, 0.0).astype(BF16)
    zero = jnp.zeros((16, 64), BF16)
    for dz in range(3):
        for slot in range(2):
            rows = []
            for dx in range(4):
                for at in range(4):
                    dy = at - slot
                    rows.append(ck_ref[dx, dy, dz] if dx < 3 and 0 <= dy < 3 else zero)
            at = 128 * dz + 64 * slot
            w4_ref[at : at + 64] = dot_t(eye, jnp.concatenate(rows, 0)).astype(BF16)


def returned_kernel(got_ref, ck_ref, pooled_ref, own_ref, near_ref, far_ref):
    _, odd = position()
    near_ref[0:18] = pooled_ref[...]
    far_ref[0:18] = pooled_ref[...]
    w1 = returned_weights(ck_ref)
    for pair in range(8):
        window = got_ref[:, 2 * pair : 2 * pair + 4].reshape(256, 128)
        product = dot(w1, window).reshape(2, 3, 3, 16, 128)
        for slot in range(2):
            low, own, high = [
                moved(product[slot, tx, 0], -1) + product[slot, tx, 1] + moved(product[slot, tx, 2], 1) for tx in range(3)
            ]
            own_ref[2 * pair + slot] = own
            near_ref[18 + 2 * pair + slot] = jnp.where(odd == 0, high, low).astype(BF16)
            far_ref[18 + 2 * pair + slot] = jnp.where(odd == 0, low, high).astype(BF16)


def window_of(refs, start, count):
    return jnp.concatenate([r[pl.ds(start, 4)].reshape(64, r.shape[-1]) for r in refs][:count], 0)


def planes_of(ref):
    return [ref.at[x] for x in range(4)]


def fine_kernel_body(a_ref, b_ref, c_ref, d_ref, w2_ref, pooled_ref, mask_ref, all_ref, sums):
    fil, odd = position()
    for k, v_ref in enumerate((a_ref, b_ref, c_ref, d_ref)):
        all_ref[k + odd * (3 - 2 * k)] = v_ref[...]

    def block(b):
        window = window_of(planes_of(all_ref), 2 * b, 4)
        product = dot(w2_ref[...], window)
        preact = moved(product[0:64], 1) + product[64:128] + moved(product[128:192], -1)
        act = jnp.maximum(preact, 0.0)
        sums[b] = (act[0:16] + act[16:32]) + (act[32:48] + act[48:64])
        return preact

    block(0)
    block(17)

    def step(b, carry):
        mask_ref[b - 1] = jnp.where(block(b) > 0, 1.0, 0.0).astype(BF16)
        return carry

    lax.fori_loop(1, 17, step, 0, unroll=True)

    @pl.when(fil == 0)
    def _():
        sums[0] = jnp.zeros((16, 256), F32)

    @pl.when(fil == 3)
    def _():
        sums[17] = jnp.zeros((16, 256), F32)

    total = sums[...].reshape(288, 256)
    high = total.astype(BF16)
    low = (total - high.astype(F32)).astype(BF16)
    pool = jnp.where(iota((256, 128), 0) // 2 == iota((256, 128), 1), 0.125, 0.0).astype(BF16)
    pooled_ref[...] = (dot(high, pool) + dot(low, pool)).astype(BF16).reshape(18, 16, 128)


def fine_grad_part(own_ref, near_msg, far_msg, all_ref, mask_ref, out_ref, up, acc):
    total = own_ref[...] + (near_msg[18:34].astype(F32) + far_msg[18:34].astype(F32))
    scaled = (total * 0.125).astype(BF16).reshape(256, 128)
    spread = jnp.where(iota((128, 256), 0) == iota((128, 256), 1) // 2, 1.0, 0.0).astype(BF16)
    up[...] = dot(scaled, spread).reshape(16, 16, 256)
    acc[...] = jnp.zeros_like(acc)

    def step(y, carry):
        row = up[y]
        cot = jnp.concatenate([row] * 4, 0) * mask_ref[y].astype(F32)
        left = jnp.concatenate([moved(cot, -1), cot, moved(cot, 1)], 0).astype(BF16)
        window = window_of(planes_of(all_ref), 2 * y + 2, 4)
        acc[...] += dot_t(left, window)
        return carry

    lax.fori_loop(0, 16, step, 0, unroll=True)
    for t in range(3):
        total = None
        for cell in range(4):
            part = roll_left(acc[64 * t + 16 * cell : 64 * t + 16 * cell + 16], 64 * (cell // 2) + 16 * (cell % 2))
            total = part if total is None else total + part
        out_ref[16 * t : 16 * t + 16] = total


def last_kernel(
    own_r, near_msg, own_msg, far_msg, got_ref, all_ref, mask_ref, w4_ref,
    out0_ref, out1_ref, out2_ref, out3_ref, grad_ref, rows_out, acc, slab, up, fine_acc, fine_ref,
):
    fil, odd = position()
    fine_grad_part(own_r, near_msg, far_msg, all_ref, mask_ref, fine_ref, up, fine_acc)
    slab[2 - 2 * odd] = near_msg[0:18]
    slab[1] = own_msg[0:18]
    slab[2 * odd] = far_msg[0:18]
    acc[...] = jnp.zeros_like(acc)
    pad = jnp.zeros((64, 128), BF16)

    def step(pair, carry):
        window = jnp.concatenate([window_of([slab.at[x] for x in range(3)], 2 * pair, 3), pad], 0)
        product = dot(w4_ref[...], window)
        result = moved(product[0:128], 1) + product[128:256] + moved(product[256:384], -1)
        result = result.astype(BF16).reshape(2, 4, 16, 128)
        for dest in range(4):
            rows_out[dest, pl.ds(2 * pair, 2)] = result[:, dest]
        cot = jnp.concatenate([got_ref[:, 2 * pair + 1 + s].reshape(64, 128) for s in range(2)], 0).astype(F32)
        left = jnp.concatenate([moved(cot, -1), cot, moved(cot, 1)], 0).astype(BF16)
        acc[...] += dot_t(left, window)
        return carry

    lax.fori_loop(0, 8, step, 0, unroll=True)
    swap = swap_matrix()
    for k, out_ref in enumerate((out0_ref, out1_ref, out2_ref, out3_ref)):
        block = rows_out[lax.bitwise_xor(fil, k)].reshape(256, 128)
        out_ref[...] = dot(swap, block).astype(BF16).reshape(16, 16, 128)
    grad_ref[0:48] = fine_ref[...].astype(BF16)
    for t in range(3):
        total = acc[128 * t : 128 * t + 64] + roll_left(acc[128 * t + 64 : 128 * t + 128], 16)
        grad_ref[48 + 64 * t : 112 + 64 * t] = total.astype(BF16)
    grad_ref[240:256] = jnp.zeros((16, 256), BF16)


def sum_kernel(parts_ref, out_ref):
    total = parts_ref[0].astype(F32)
    for src in range(1, 16):
        total = total + parts_ref[src].astype(F32)
    for dest in range(16):
        out_ref[dest] = total.astype(BF16)


def unpack_kernel(grad_ref, got0_ref, got1_ref, got2_ref, got3_ref, fine_ref, coarse_ref, out_ref):
    fil, _ = position()
    eye = jnp.where(iota((256, 256), 0) == iota((256, 256), 1), 1.0, 0.0).astype(BF16)
    for dz in range(3):
        block = grad_ref[dz].astype(F32)
        columns = dot_t(eye, grad_ref[3 + 4 * dz : 7 + 4 * dz].reshape(64, 256))
        for dx in range(3):
            for dy in range(3):
                at = 64 * dx + 16 * dy
                fine_ref[dx, dy, dz] = roll_left(block, at)[:, 0:16]
                coarse_ref[dx, dy, dz] = columns[at : at + 16]
    for k, got_ref in enumerate((got0_ref, got1_ref, got2_ref, got3_ref)):
        at = pl.multiple_of(16 * lax.bitwise_xor(fil, k), 16)
        out_ref[:, 0, pl.ds(at, 16), :] = got_ref[...]


def swapped(near, far):
    count = lax.axis_size("vox")
    first = [(i, i ^ 1) for i in range(count)]
    second = [(i, ((i + 1) ^ 1) - 1) for i in range(1, count - 1)]
    near = lax.ppermute(near, "vox", first)
    far = lax.ppermute(far, "vox", second)
    return near, far


def exchange(pieces, groups):
    return lax.all_to_all(pieces, ("vox", "fil"), 0, 0, tiled=True, axis_index_groups=groups)


def local(volume, fine_kernel, coarse_kernel, coarse_cot):
    plane, edge, wide = ((32, 16, 256), BF16), ((6, 16, 256), BF16), ((38, 16, 256), BF16)
    near, far, edge1, edge3 = call(
        pack_kernel,
        [plane, plane, edge, edge],
        scratch=[pltpu.VMEM(volume.shape, BF16), pltpu.SemaphoreType.DMA((1,))],
        n_in=1,
        spec=HBM,
    )(volume)
    (pay,) = call(pack_cot_kernel, [((4, 18, 16, 128), BF16)], n_in=1, unread=1)(coarse_cot, edge1)
    edge1 = lax.ppermute(edge1, "fil", [(i, i ^ 1) for i in range(4)])
    edge3 = lax.ppermute(edge3, "fil", [(1, 2), (2, 1)])
    got = lax.all_to_all(pay, "fil", 0, 0, tiled=True)
    near, far = call(extend_kernel, [wide, wide], n_in=4)(near, far, edge1, edge3)
    near_got, far_got = swapped(near, far)
    (w2,) = call(fine_weights_kernel, [((192, 256), BF16)], n_in=1)(fine_kernel.transpose(2, 3, 4, 0, 1))
    coarse_taps = coarse_kernel.transpose(2, 3, 4, 1, 0)
    pooled, mask, cells = call(
        fine_kernel_body,
        [((18, 16, 128), BF16), ((16, 64, 256), BF16), ((4, 38, 16, 256), BF16)],
        scratch=[pltpu.VMEM((18, 16, 256), F32)],
        n_in=5,
    )(far_got, far, near, near_got, w2)
    message = ((34, 16, 128), BF16)
    own_r, near_msg, far_msg = call(
        returned_kernel, [((16, 16, 128), F32), message, message], n_in=3
    )(got, coarse_taps, pooled)
    (w4,) = call(coarse_weights_kernel, [((384, 256), BF16)], n_in=1, unread=1)(coarse_taps, near_msg)
    near_msg_got, far_msg_got = swapped(near_msg, far_msg)
    *out_pieces, grads = call(
        last_kernel,
        [((16, 16, 128), BF16)] * 4 + [((256, 256), BF16)],
        scratch=[
            pltpu.VMEM((4, 16, 16, 128), BF16),
            pltpu.VMEM((384, 256), F32),
            pltpu.VMEM((3, 18, 16, 128), BF16),
            pltpu.VMEM((16, 16, 256), F32),
            pltpu.VMEM((192, 256), F32),
            pltpu.VMEM((48, 256), F32),
        ],
        n_in=8,
    )(own_r, near_msg_got, near_msg, far_msg_got, got, cells, mask, w4)
    out_got = out_pieces[:1] + [
        lax.ppermute(out_pieces[k], "fil", [(i, i ^ k) for i in range(4)]) for k in range(1, 4)
    ]
    lines = [[16 * g + j for j in range(16)] for g in range(16)]
    sheets = [[16 * g + j for g in range(16)] for j in range(16)]
    summed = call(sum_kernel, [((16, 16, 256), BF16)])
    parts = exchange(grads.reshape(16, 16, 256), sheets)
    parts = exchange(summed(parts)[0], lines)
    spread = exchange(summed(parts)[0], sheets)
    grad_fine, grad_coarse, coarse_out = call(
        unpack_kernel, [((3, 3, 3, 16, 16), F32), ((3, 3, 3, 16, 64), F32), ((16, 1, 64, 128), BF16)], n_in=5
    )(spread, *out_got)
    return (coarse_out, grad_fine.transpose(3, 4, 0, 1, 2), grad_coarse.transpose(4, 3, 0, 1, 2))


def solution(mesh):
    in_specs = (P(None, "vox", "fil", None), P(), P(), P("fil", "vox", None, None))
    out_specs = (P("fil", "vox", None, None), P(), P())
    return jax.shard_map(local, mesh=mesh, in_specs=in_specs, out_specs=out_specs, check_vma=False)
```

```python
import jax
import jax.numpy as jnp
from jax import lax
from jax.experimental import pallas as pl
from jax.experimental.pallas import tpu as pltpu
from jax.sharding import PartitionSpec as P


F32 = jnp.float32
BF16 = jnp.bfloat16
VMEM = pl.BlockSpec(memory_space=pltpu.VMEM)
HBM = pl.BlockSpec(memory_space=pltpu.HBM)


def dot(a, b):
    return lax.dot_general(a, b, (((1,), (0,)), ((), ())), preferred_element_type=F32)


def dot_t(a, b):
    return lax.dot_general(a, b, (((1,), (1,)), ((), ())), preferred_element_type=F32)


def iota(shape, dim):
    return lax.broadcasted_iota(jnp.int32, shape, dim)


def position():
    return lax.axis_index("fil"), lax.rem(lax.axis_index("vox"), 2)


def swap_matrix():
    row, col = iota((256, 256), 0), iota((256, 256), 1)
    return jnp.where(col == (row % 16) * 16 + row // 16, 1.0, 0.0).astype(BF16)


def roll_left(x, amount):
    return x if amount == 0 else pltpu.roll(x, x.shape[1] - amount, 1)


def moved(x, step):
    if step == 0:
        return x
    width = x.shape[1]
    edge = 0 if step == 1 else width - 1
    return jnp.where(iota(x.shape, 1) == edge, 0.0, pltpu.roll(x, step % width, 1))


def call(body, outs, scratch=(), flops=2_000_000_000, n_in=1, spec=VMEM, unread=0, vmem=32 * 1024 * 1024):
    specs = [spec] * n_in + [pl.BlockSpec(memory_space=pl.ANY)] * unread
    return pl.pallas_call(
        body,
        out_shape=tuple(jax.ShapeDtypeStruct(s, d) for s, d in outs),
        in_specs=specs,
        out_specs=tuple(VMEM for _ in outs),
        scratch_shapes=scratch,
        cost_estimate=pl.CostEstimate(flops=flops, bytes_accessed=1_000_000, transcendentals=0),
        compiler_params=pltpu.CompilerParams(vmem_limit_bytes=vmem),
    )


def pack_kernel(vol_hbm, near_ref, far_ref, edge1_ref, edge3_ref, vol_ref, sem):
    fil, odd = position()
    load = pltpu.make_async_copy(vol_hbm, vol_ref, sem.at[0])
    load.start()
    swap = swap_matrix()
    load.wait()
    for which, v_ref in enumerate((near_ref, far_ref)):
        x = 1 - odd if which == 0 else odd
        for half in range(2):
            block = vol_ref[:, pl.ds(x, 1), 16 * half : 16 * half + 16, :].reshape(256, 256)
            v_ref[16 * half : 16 * half + 16] = dot(swap, block).astype(BF16).reshape(16, 16, 256)
        low, high = v_ref[0:3], v_ref[29:32]
        edge1_ref[3 * which : 3 * which + 3] = jnp.where(lax.rem(fil, 2) == 0, high, low)
        edge3_ref[3 * which : 3 * which + 3] = jnp.where(fil < 2, high, low)


def pack_cot_kernel(cot_ref, after_ref, pay_ref):
    swap = swap_matrix()
    for dest in range(4):
        block = cot_ref[:, 0, 16 * dest : 16 * dest + 16, :].reshape(256, 128)
        rows = dot(swap, block).astype(BF16).reshape(16, 16, 128)
        pay_ref[dest, 1:17] = rows
        if dest < 3:
            pay_ref[dest + 1, 0] = rows[15]
        else:
            pay_ref[0, 0] = jnp.zeros((16, 128), BF16)
        if dest > 0:
            pay_ref[dest - 1, 17] = rows[0]
        else:
            pay_ref[3, 17] = jnp.zeros((16, 128), BF16)


def extend_kernel(near_ref, far_ref, edge1_ref, edge3_ref, near_out, far_out):
    fil, _ = position()
    upper = lax.rem(fil, 2) == 1
    for which, (v_ref, out_ref) in enumerate(((near_ref, near_out), (far_ref, far_out))):
        rows = slice(3 * which, 3 * which + 3)
        out_ref[3:35] = v_ref[...]
        out_ref[0:3] = jnp.where(upper, edge1_ref[rows], edge3_ref[rows])
        out_ref[35:38] = jnp.where(upper, edge3_ref[rows], edge1_ref[rows])


def returned_weights(ck_ref):
    row, col = iota((64, 256), 0), iota((64, 256), 1)
    slots = []
    for slot in range(2):
        total = None
        for dy in range(3):
            place = jnp.where(col == (row // 16) * 64 + (slot + 2 - dy) * 16 + row % 16, 1.0, 0.0).astype(BF16)
            part = dot(ck_ref[:, dy].reshape(144, 64), place)
            total = part if total is None else total + part
        slots.append(total.astype(BF16))
    return jnp.concatenate(slots, 0)


def fine_weights_kernel(fk_ref, w2_ref):
    row, col = iota((16, 256), 0), iota((16, 256), 1)
    total = None
    for dx in range(3):
        for dy in range(3):
            place = jnp.where(col == row + 64 * dx + 16 * dy, 1.0, 0.0).astype(BF16)
            part = dot(fk_ref[dx, dy].reshape(48, 16), place)
            total = part if total is None else total + part
    for x in range(2):
        for y in range(2):
            amount = 64 * x + 16 * y
            rolled = (pltpu.roll(total, amount, 1) if amount else total).astype(BF16)
            for dz in range(3):
                at = 64 * dz + 32 * x + 16 * y
                w2_ref[at : at + 16] = rolled[16 * dz : 16 * dz + 16]


def coarse_weights_kernel(ck_ref, after_ref, w4_ref):
    eye = jnp.where(iota((64, 64), 0) == iota((64, 64), 1), 1.0, 0.0).astype(BF16)
    zero = jnp.zeros((16, 64), BF16)
    for dz in range(3):
        for slot in range(2):
            rows = []
            for dx in range(4):
                for at in range(4):
                    dy = at - slot
                    rows.append(ck_ref[dx, dy, dz] if dx < 3 and 0 <= dy < 3 else zero)
            at = 128 * dz + 64 * slot
            w4_ref[at : at + 64] = dot_t(eye, jnp.concatenate(rows, 0)).astype(BF16)


def returned_kernel(got_ref, ck_ref, pooled_ref, own_ref, near_ref, far_ref):
    _, odd = position()
    near_ref[0:18] = pooled_ref[...]
    far_ref[0:18] = pooled_ref[...]
    w1 = returned_weights(ck_ref)
    for pair in range(8):
        window = got_ref[:, 2 * pair : 2 * pair + 4].reshape(256, 128)
        product = dot(w1, window).reshape(2, 3, 3, 16, 128)
        for slot in range(2):
            low, own, high = [
                moved(product[slot, tx, 0], -1) + product[slot, tx, 1] + moved(product[slot, tx, 2], 1) for tx in range(3)
            ]
            own_ref[2 * pair + slot] = own
            near_ref[18 + 2 * pair + slot] = jnp.where(odd == 0, high, low).astype(BF16)
            far_ref[18 + 2 * pair + slot] = jnp.where(odd == 0, low, high).astype(BF16)


def window_of(refs, start, count):
    return jnp.concatenate([r[pl.ds(start, 4)].reshape(64, r.shape[-1]) for r in refs][:count], 0)


def planes_of(ref):
    return [ref.at[x] for x in range(4)]


def fine_kernel_body(a_ref, b_ref, c_ref, d_ref, w2_ref, pooled_ref, mask_ref, all_ref, sums):
    fil, odd = position()
    for k, v_ref in enumerate((a_ref, b_ref, c_ref, d_ref)):
        all_ref[k + odd * (3 - 2 * k)] = v_ref[...]

    def block(b):
        window = window_of(planes_of(all_ref), 2 * b, 4)
        product = dot(w2_ref[...], window)
        preact = moved(product[0:64], 1) + product[64:128] + moved(product[128:192], -1)
        act = jnp.maximum(preact, 0.0)
        sums[b] = (act[0:16] + act[16:32]) + (act[32:48] + act[48:64])
        return preact

    block(0)
    block(17)

    def step(b, carry):
        mask_ref[b - 1] = jnp.where(block(b) > 0, 1.0, 0.0).astype(BF16)
        return carry

    lax.fori_loop(1, 17, step, 0, unroll=True)

    @pl.when(fil == 0)
    def _():
        sums[0] = jnp.zeros((16, 256), F32)

    @pl.when(fil == 3)
    def _():
        sums[17] = jnp.zeros((16, 256), F32)

    total = sums[...].reshape(288, 256)
    high = total.astype(BF16)
    low = (total - high.astype(F32)).astype(BF16)
    pool = jnp.where(iota((256, 128), 0) // 2 == iota((256, 128), 1), 0.125, 0.0).astype(BF16)
    pooled_ref[...] = (dot(high, pool) + dot(low, pool)).astype(BF16).reshape(18, 16, 128)


def fine_grad_part(own_ref, near_msg, far_msg, all_ref, mask_ref, out_ref, up, acc):
    total = own_ref[...] + (near_msg[18:34].astype(F32) + far_msg[18:34].astype(F32))
    scaled = (total * 0.125).astype(BF16).reshape(256, 128)
    spread = jnp.where(iota((128, 256), 0) == iota((128, 256), 1) // 2, 1.0, 0.0).astype(BF16)
    up[...] = dot(scaled, spread).reshape(16, 16, 256)
    for group in range(4):
        lefts, windows = [], []
        for y in range(4 * group, 4 * group + 4):
            cot = jnp.concatenate([up[y]] * 4, 0) * mask_ref[y].astype(F32)
            lefts.append(jnp.concatenate([moved(cot, -1), cot, moved(cot, 1)], 0).astype(BF16))
            windows.append(window_of(planes_of(all_ref), 2 * y + 2, 4))
        part = dot_t(jnp.concatenate(lefts, 1), jnp.concatenate(windows, 1))
        acc[...] = part if group == 0 else acc[...] + part
    for t in range(3):
        total = None
        for cell in range(4):
            part = roll_left(acc[64 * t + 16 * cell : 64 * t + 16 * cell + 16], 64 * (cell // 2) + 16 * (cell % 2))
            total = part if total is None else total + part
        out_ref[16 * t : 16 * t + 16] = total


def last_kernel(
    own_r, near_msg, own_msg, far_msg, got_ref, all_ref, mask_ref, w4_ref,
    out0_ref, out1_ref, out2_ref, out3_ref, grad_ref, rows_out, acc, slab, up, fine_acc, fine_ref,
):
    fil, odd = position()
    fine_grad_part(own_r, near_msg, far_msg, all_ref, mask_ref, fine_ref, up, fine_acc)
    slab[2 - 2 * odd] = near_msg[0:18]
    slab[1] = own_msg[0:18]
    slab[2 * odd] = far_msg[0:18]
    pad = jnp.zeros((64, 128), BF16)
    for group in range(2):
        lefts, windows = [], []
        for pair in range(4 * group, 4 * group + 4):
            window = jnp.concatenate([window_of([slab.at[x] for x in range(3)], 2 * pair, 3), pad], 0)
            product = dot(w4_ref[...], window)
            result = moved(product[0:128], 1) + product[128:256] + moved(product[256:384], -1)
            result = result.astype(BF16).reshape(2, 4, 16, 128)
            for dest in range(4):
                rows_out[dest, 2 * pair : 2 * pair + 2] = result[:, dest]
            cot = jnp.concatenate([got_ref[:, 2 * pair + 1 + s].reshape(64, 128) for s in range(2)], 0).astype(F32)
            lefts.append(jnp.concatenate([moved(cot, -1), cot, moved(cot, 1)], 0).astype(BF16))
            windows.append(window)
        part = dot_t(jnp.concatenate(lefts, 1), jnp.concatenate(windows, 1))
        acc[...] = part if group == 0 else acc[...] + part
    swap = swap_matrix()
    for k, out_ref in enumerate((out0_ref, out1_ref, out2_ref, out3_ref)):
        block = rows_out[lax.bitwise_xor(fil, k)].reshape(256, 128)
        out_ref[...] = dot(swap, block).astype(BF16).reshape(16, 16, 128)
    grad_ref[0:48] = fine_ref[...].astype(BF16)
    for t in range(3):
        total = acc[128 * t : 128 * t + 64] + roll_left(acc[128 * t + 64 : 128 * t + 128], 16)
        grad_ref[48 + 64 * t : 112 + 64 * t] = total.astype(BF16)
    grad_ref[240:256] = jnp.zeros((16, 256), BF16)


def sum_kernel(parts_ref, out_ref):
    total = parts_ref[0].astype(F32)
    for src in range(1, 16):
        total = total + parts_ref[src].astype(F32)
    for dest in range(16):
        out_ref[dest] = total.astype(BF16)


def unpack_kernel(grad_ref, got0_ref, got1_ref, got2_ref, got3_ref, fine_ref, coarse_ref, out_ref):
    fil, _ = position()
    eye = jnp.where(iota((256, 256), 0) == iota((256, 256), 1), 1.0, 0.0).astype(BF16)
    for dz in range(3):
        block = grad_ref[dz].astype(F32)
        columns = dot_t(eye, grad_ref[3 + 4 * dz : 7 + 4 * dz].reshape(64, 256))
        for dx in range(3):
            for dy in range(3):
                at = 64 * dx + 16 * dy
                fine_ref[dx, dy, dz] = roll_left(block, at)[:, 0:16]
                coarse_ref[dx, dy, dz] = columns[at : at + 16]
    for k, got_ref in enumerate((got0_ref, got1_ref, got2_ref, got3_ref)):
        at = pl.multiple_of(16 * lax.bitwise_xor(fil, k), 16)
        out_ref[:, 0, pl.ds(at, 16), :] = got_ref[...]


def swapped(near, far):
    count = lax.axis_size("vox")
    first = [(i, i ^ 1) for i in range(count)]
    second = [(i, ((i + 1) ^ 1) - 1) for i in range(1, count - 1)]
    near = lax.ppermute(near, "vox", first)
    far = lax.ppermute(far, "vox", second)
    return near, far


def exchange(pieces, groups):
    return lax.all_to_all(pieces, ("vox", "fil"), 0, 0, tiled=True, axis_index_groups=groups)


def local(volume, fine_kernel, coarse_kernel, coarse_cot):
    plane, edge, wide = ((32, 16, 256), BF16), ((6, 16, 256), BF16), ((38, 16, 256), BF16)
    near, far, edge1, edge3 = call(
        pack_kernel,
        [plane, plane, edge, edge],
        scratch=[pltpu.VMEM(volume.shape, BF16), pltpu.SemaphoreType.DMA((1,))],
        n_in=1,
        spec=HBM,
    )(volume)
    (pay,) = call(pack_cot_kernel, [((4, 18, 16, 128), BF16)], n_in=1, unread=1)(coarse_cot, edge1)
    edge1 = lax.ppermute(edge1, "fil", [(i, i ^ 1) for i in range(4)])
    edge3 = lax.ppermute(edge3, "fil", [(1, 2), (2, 1)])
    got = lax.all_to_all(pay, "fil", 0, 0, tiled=True)
    near, far = call(extend_kernel, [wide, wide], n_in=4)(near, far, edge1, edge3)
    near_got, far_got = swapped(near, far)
    (w2,) = call(fine_weights_kernel, [((192, 256), BF16)], n_in=1)(fine_kernel.transpose(2, 3, 4, 0, 1))
    coarse_taps = coarse_kernel.transpose(2, 3, 4, 1, 0)
    pooled, mask, cells = call(
        fine_kernel_body,
        [((18, 16, 128), BF16), ((16, 64, 256), BF16), ((4, 38, 16, 256), BF16)],
        scratch=[pltpu.VMEM((18, 16, 256), F32)],
        n_in=5,
    )(far_got, far, near, near_got, w2)
    message = ((34, 16, 128), BF16)
    own_r, near_msg, far_msg = call(
        returned_kernel, [((16, 16, 128), F32), message, message], n_in=3
    )(got, coarse_taps, pooled)
    (w4,) = call(coarse_weights_kernel, [((384, 256), BF16)], n_in=1, unread=1)(coarse_taps, near_msg)
    near_msg_got, far_msg_got = swapped(near_msg, far_msg)
    *out_pieces, grads = call(
        last_kernel,
        [((16, 16, 128), BF16)] * 4 + [((256, 256), BF16)],
        scratch=[
            pltpu.VMEM((4, 16, 16, 128), BF16),
            pltpu.VMEM((384, 256), F32),
            pltpu.VMEM((3, 18, 16, 128), BF16),
            pltpu.VMEM((16, 16, 256), F32),
            pltpu.VMEM((192, 256), F32),
            pltpu.VMEM((48, 256), F32),
        ],
        n_in=8,
    )(own_r, near_msg_got, near_msg, far_msg_got, got, cells, mask, w4)
    out_got = out_pieces[:1] + [
        lax.ppermute(out_pieces[k], "fil", [(i, i ^ k) for i in range(4)]) for k in range(1, 4)
    ]
    lines = [[16 * g + j for j in range(16)] for g in range(16)]
    sheets = [[16 * g + j for g in range(16)] for j in range(16)]
    summed = call(sum_kernel, [((16, 16, 256), BF16)])
    parts = exchange(grads.reshape(16, 16, 256), sheets)
    parts = exchange(summed(parts)[0], lines)
    spread = exchange(summed(parts)[0], sheets)
    grad_fine, grad_coarse, coarse_out = call(
        unpack_kernel, [((3, 3, 3, 16, 16), F32), ((3, 3, 3, 16, 64), F32), ((16, 1, 64, 128), BF16)], n_in=5
    )(spread, *out_got)
    return (coarse_out, grad_fine.transpose(3, 4, 0, 1, 2), grad_coarse.transpose(4, 3, 0, 1, 2))


def solution(mesh):
    in_specs = (P(None, "vox", "fil", None), P(), P(), P("fil", "vox", None, None))
    out_specs = (P("fil", "vox", None, None), P(), P())
    return jax.shard_map(local, mesh=mesh, in_specs=in_specs, out_specs=out_specs, check_vma=False)
```
